32 devices in a mesh: blk: 4 (over y, x), half: 2 (over core), rep: 4 (over z).
Axes of the slice: x: 2, y: 2, z: 4, core: 2. Of those that a mesh axis runs over, the one named last changes fastest.
Arguments:
- tokens: bfloat16 [1024, 2048], P('blk'), may hold values from -6 to 6
- experts: int32 [1024, 6], P('blk'), may hold values from 0 to 63, all different within a row; in each aligned block of 256 rows (0 to 255, 256 to 511, ...) at most 32 rows name the same one
- gates: bfloat16 [1024, 6], P('blk'), may hold values from 0.099609375 to 1
- w_gate: bfloat16 [64, 1408, 2048], P('blk', ('half', 'rep')), may hold values from -0.125 to 0.125
- w_up: bfloat16 [64, 1408, 2048], P('blk', ('half', 'rep')), may hold values from -0.125 to 0.125
- w_down: bfloat16 [64, 1408, 2048], P('blk', ('half', 'rep')), may hold values from -0.15625 to 0.15625
- shared_gate: bfloat16 [1408, 2048], P(('half', 'rep')), may hold values from -0.125 to 0.125
- shared_up: bfloat16 [1408, 2048], P(('half', 'rep')), may hold values from -0.125 to 0.125
- shared_down: bfloat16 [1408, 2048], P(('half', 'rep')), may hold values from -0.15625 to 0.15625
Outputs:
- mixed: bfloat16 [1024, 2048], P('blk', ('half', 'rep'))
The draws below stay inside these ranges and needn't reach their ends.
Inputs may be any that keep to these rules, and one draw needn't show every extreme that they name: Each row names 6 different experts. Among the 256 rows held by one index of blk no expert is named by more than 32 rows, a bound that some block reaches.
All inputs are finite; a program needn't handle non-finite values.
Results may differ from the reference program's by a relative error of at most 0.0055.
Values may be sent and summed in bfloat16 or wider, within the bound.
A program may use at most 128 MiB of HBM per device.

```python
import math
import jax
import jax.numpy as jnp
import numpy as np
from jax import lax

D = 2048
FF = 1408
E = 64
TOPK = 6
SH = 1408
TOK_DEV = 256
TOKENS = 1024
CAP = 32
N_BLK = 4
N_HALF = 2


def steps_of(stream_key, shape, shards, low, top_value):
    def one(dim, shards_of):
        draws = jax.random.uniform(jax.random.fold_in(jax.random.fold_in(stream_key, 6), dim), (shards_of,), jnp.float32, low / len(shards), top_value / len(shards))
        return jnp.repeat(jnp.exp(draws), shape[dim] // shards_of).reshape((-1,) + (1,) * (len(shape) - dim - 1))

    factor_of = one(*shards[0])
    for cut in shards[1:]:
        factor_of = factor_of * one(*cut)
    return factor_of


def routed_block(own_key, own, number, rows, amount, top, bound, slope):
    ranking = jax.random.permutation(own_key, amount)
    packed, common = shares(amount, rows * top, bound, slope, True), shares(amount, rows * top, bound, slope, False)
    places = jnp.arange(amount)

    def named(sizes, rotation):
        used = int((sizes > 0).sum())
        fixed = max(1, used // 4)
        moved = fixed + (places - fixed + rotation * (used - fixed)) % max(1, amount - fixed)
        return jnp.zeros((amount,), jnp.int32).at[ranking[jnp.where(places < fixed, places, moved)]].set(jnp.asarray(sizes, jnp.int32))

    sizes = jnp.where(number % 4 == 0, named(packed, number // 4), named(common, number - number // 4 - 1))
    mixed = jax.random.permutation(jax.random.fold_in(own, 3), amount)
    source_of, taker = mixed[0:amount // 2 * 2:2], mixed[1:amount // 2 * 2:2]
    margin = jnp.minimum(sizes[source_of] - 1, bound - sizes[taker]) // 2
    margin = jnp.where((source_of == ranking[0]) | (taker == ranking[0]) | (sizes[taker] == 0), 0, jnp.maximum(margin, 0))
    moved = jax.random.randint(jax.random.fold_in(own, 4), (amount // 2,), 0, 1 << 20) % (margin + 1)
    sizes = sizes.at[source_of].add(-moved).at[taker].add(moved)
    members = jnp.searchsorted(jnp.cumsum(sizes), jnp.arange(rows * top), side="right").astype(jnp.int32)
    listing = members.reshape(top, rows).T
    listing = listing[jax.random.permutation(jax.random.fold_in(own, 1), rows)]
    rotation = jax.random.randint(jax.random.fold_in(own, 2), (rows, 1), 0, top)
    return jnp.take_along_axis(listing, (jnp.arange(top)[None, :] + rotation) % top, axis=1)


def shares(amount, total, most, slope, full):
    weights = [(1 << 20) // math.isqrt(rank ** slope) + 1 for rank in range(1, amount + 1)]
    largest = most if full else min(most, max(-(-total // amount), total * weights[0] // sum(weights)))
    least = 1 if total - largest >= amount - 1 else 0
    counts, spare = [largest] + [least] * (amount - 1), total - largest - least * (amount - 1)
    while spare > 0:
        candidates = [i for i in range(1, amount) if counts[i] < largest] or [i for i in range(1, amount) if counts[i] < most]
        mass, remaining = sum([weights[i] for i in candidates]), spare
        for i in candidates:
            more = min(most - counts[i], max(1, remaining * weights[i] // mass), spare)
            counts[i] = counts[i] + more
            spare = spare - more
    return np.array(counts)


def noise(rng, shape, deviation, bound, shards=(), kind=jnp.bfloat16):
    values = deviation * jax.random.normal(rng, shape, jnp.float32)
    if shards:
        values = values * steps_of(rng, shape, shards, -0.22, 0.18)
    return jnp.clip(values, -bound, bound).astype(kind)


def setup_inputs(seed: int = 0) -> dict:
    key_list = jax.random.split(jax.random.key(seed), 10)
    tokens = noise(key_list[0], (TOKENS, D), 1.0, 6.0, ((0, 4),))
    experts_keys = jax.random.split(jax.random.fold_in(key_list[1], 1), TOKENS // TOK_DEV)
    experts_turns = jax.random.permutation(jax.random.fold_in(key_list[1], 3), TOKENS // TOK_DEV)
    experts = jax.vmap(lambda own, number: routed_block(jax.random.fold_in(key_list[1], 2), own, number, TOK_DEV, E, TOPK, CAP, 1))(experts_keys, experts_turns).reshape((TOKENS, TOPK))
    gates = jnp.clip(jnp.exp(math.log(1.0) - 2.306499 * jax.random.uniform(key_list[2], (TOKENS, TOPK), jnp.float32) ** steps_of(key_list[2], (TOKENS, TOPK), ((0, 4),), -0.2, 0.2)), 0.099609375, 1.0).astype(jnp.bfloat16)
    w_gate = noise(key_list[3], (E, FF, D), D ** -0.5, 0.125, ((0, 4), (1, 8)))
    w_up = noise(key_list[4], (E, FF, D), D ** -0.5, 0.125, ((0, 4), (1, 8)))
    w_down = noise(key_list[5], (E, FF, D), FF ** -0.5, 0.15625, ((0, 4), (1, 8)))
    shared_gate = noise(key_list[6], (SH, D), D ** -0.5, 0.125, ((0, 8),))
    shared_up = noise(key_list[7], (SH, D), D ** -0.5, 0.125, ((0, 8),))
    shared_down = noise(key_list[8], (SH, D), SH ** -0.5, 0.15625, ((0, 8),))
    return dict(tokens=tokens, experts=experts, gates=gates, w_gate=w_gate, w_up=w_up, w_down=w_down, shared_gate=shared_gate, shared_up=shared_up, shared_down=shared_down)


def reference(tokens, experts, gates, w_gate, w_up, w_down, shared_gate, shared_up, shared_down):
    blocks = N_HALF
    block_width = FF // blocks
    pairs = TOK_DEV * TOPK
    grouped = experts.reshape(N_BLK, pairs)
    onehot = (grouped[:, :, None] == jnp.arange(E, dtype=jnp.int32)[None, None, :]).astype(jnp.int32)
    before = jnp.cumsum(onehot, axis=1) - onehot
    ranks = jnp.sum(before * onehot, axis=2).astype(jnp.int32)
    source = jnp.arange(N_BLK, dtype=jnp.int32)[:, None]
    position = source * CAP + ranks
    token_ids = source * TOK_DEV + (jnp.arange(pairs, dtype=jnp.int32) // TOPK)[None, :]
    table = jnp.full((E, N_BLK * CAP), TOKENS, jnp.int32)
    table = table.at[grouped.reshape(-1), position.reshape(-1)].set(token_ids.reshape(-1).astype(jnp.int32))
    weight_table = jnp.zeros((E, N_BLK * CAP), jnp.float32)
    weight_table = weight_table.at[grouped.reshape(-1), position.reshape(-1)].set(gates.reshape(-1).astype(jnp.float32))

    def one_expert(carry, item):
        index, weights, gate_matrix, up_weight, down_w = item
        token_rows = jnp.take(tokens, index, axis=0, mode="fill", fill_value=0)
        gate_values = jnp.dot(token_rows, gate_matrix.T, preferred_element_type=jnp.float32)
        raised_rows = jnp.dot(token_rows, up_weight.T, preferred_element_type=jnp.float32)
        hidden_state = (jax.nn.silu(gate_values) * raised_rows).astype(jnp.bfloat16)
        count = hidden_state.shape[0]
        pieces = jnp.einsum("rkf,kfd->rkd", hidden_state.reshape(count, blocks, block_width).astype(jnp.float32),
                            down_w.reshape(blocks, block_width, D).astype(jnp.float32))
        rounded = lax.optimization_barrier(pieces.astype(jnp.bfloat16))
        summed = jnp.sum(rounded.astype(jnp.float32), axis=1)
        carry = carry.at[index].add(weights[:, None] * summed, mode="drop")
        return carry, None

    routed, _ = lax.scan(one_expert, jnp.zeros((TOKENS, D), jnp.float32),
                         (table, weight_table, w_gate, w_up, w_down))
    shared_hidden = (jax.nn.silu(jnp.dot(tokens, shared_gate.T, preferred_element_type=jnp.float32))
                     * jnp.dot(tokens, shared_up.T, preferred_element_type=jnp.float32)).astype(jnp.bfloat16)
    shared_output = jnp.dot(shared_hidden, shared_down, preferred_element_type=jnp.float32)
    return (routed + shared_output).astype(jnp.bfloat16)
```

```python
import functools

import jax
import jax.numpy as jnp
from jax import lax
from jax.experimental import pallas as pl
from jax.experimental.pallas import tpu as pltpu
from jax.sharding import PartitionSpec as P

E = 64
CAP = 32


def hidden_units(token_rows, gate_matrix, up_weight):
    gate_values = jnp.einsum(
        "kan,ktn->kat", token_rows, gate_matrix, preferred_element_type=jnp.float32
    )
    raised_rows = jnp.einsum(
        "kan,ktn->kat", token_rows, up_weight, preferred_element_type=jnp.float32
    )
    return (jax.nn.silu(gate_values) * raised_rows).astype(jnp.bfloat16)


def place_slots(flat, ranks, block_size, which, slot_count):
    inside = ranks // block_size == which
    local = jnp.where(inside, flat * block_size + ranks % block_size, -1)
    return local[:, None] == jnp.arange(slot_count, dtype=jnp.int32)[None, :]


def per_device(tokens, experts, gates, w_gate, w_up, w_down, shared_gate, shared_up, shared_down):
    token_count = tokens.shape[0]
    width = tokens.shape[1]
    topk = experts.shape[1]
    exp_local = w_gate.shape[0]
    blk_count = lax.axis_size("blk")
    slot_block = CAP // lax.axis_size("rep")
    member_rep = lax.axis_index("rep")
    flat = experts.reshape(-1)
    onehot = (flat[:, None] == jnp.arange(E, dtype=jnp.int32)[None, :]).astype(jnp.int32)
    before = jnp.cumsum(onehot, axis=0) - onehot
    ranks = jnp.sum(before * onehot, axis=1)
    placing = place_slots(flat, ranks, slot_block, member_rep, E * slot_block).reshape(
        token_count, topk, -1
    )
    weighting = jnp.sum(
        placing.astype(jnp.float32) * gates.astype(jnp.float32)[:, :, None], axis=1
    ).astype(jnp.bfloat16)
    selector = jnp.any(placing, axis=1).astype(jnp.bfloat16)
    filled = jnp.einsum("ts,td->sd", selector, tokens, preferred_element_type=jnp.float32).astype(
        jnp.bfloat16
    )
    filled = filled.reshape(E, 1, slot_block, width)
    arrived = lax.all_to_all(filled, "blk", split_axis=0, concat_axis=1, tiled=True)
    token_rows = arrived.reshape(exp_local, -1, width)
    every_hidden = hidden_units(lax.all_gather(token_rows, "rep", axis=1, tiled=True), w_gate, w_up)
    mine = lax.all_to_all(every_hidden, "rep", split_axis=1, concat_axis=2, tiled=True)
    partial_value = jnp.einsum(
        "otv,ovj->otj",
        mine,
        lax.all_gather(w_down, "rep", axis=1, tiled=True),
        preferred_element_type=jnp.float32,
    )
    block_out = partial_value.astype(jnp.bfloat16).reshape(exp_local, blk_count, slot_block, width)
    returned = lax.all_to_all(block_out, "blk", split_axis=1, concat_axis=0, tiled=True)
    returned = returned.reshape(E * slot_block, width)
    routed = jnp.dot(weighting, returned, preferred_element_type=jnp.float32)
    shared_hidden = (
        jax.nn.silu(
            jnp.einsum("td,sd->ts", tokens, shared_gate, preferred_element_type=jnp.float32)
        )
        * jnp.einsum("td,sd->ts", tokens, shared_up, preferred_element_type=jnp.float32)
    ).astype(jnp.bfloat16)
    shared_output = jnp.dot(shared_hidden, shared_down, preferred_element_type=jnp.float32)
    routed_share = lax.psum_scatter(routed, ("half", "rep"), scatter_dimension=1, tiled=True)
    shared_share = lax.psum_scatter(shared_output, ("half", "rep"), scatter_dimension=1, tiled=True)
    total = routed_share + shared_share
    return total.astype(jnp.bfloat16)


BF = jnp.bfloat16
F32 = jnp.float32
NT = (((1,), (1,)), ((), ()))


def dot(a, b):
    return jnp.dot(a, b, preferred_element_type=F32)


def silu_mul(g, u):
    return (g / (1.0 + jnp.exp(-g)) * u).astype(BF)


def fused_kernel(
    tok, meta, sg, su, sd, wg, wu, wd, out,
    tokb, metab, xs, hb, hs, comb, yb, gbuf, ubuf, dbuf,
    acc, keep, dsend, drecv, asend, arecv, bsend, brecv, zsend, zrecv,
    gsem, usem, dsem, t_s, t_r, p_s, p_r, m_s, m_r, d_s, d_r, a_s, a_r, b_s, b_r, z_s, z_r,
):
    T, D = tok.shape
    el, F, _ = wg.shape
    ring = gbuf.shape[0]
    W = out.shape[1]
    reps = D // (2 * W)
    H = T // 2
    G = t_s.shape[1]
    R = H // G
    me = lax.axis_index("blk")
    c = lax.axis_index("half")
    z = lax.axis_index("rep")
    x = me % 2
    y = me // 2
    xn = y * 2 + (1 - x)
    yn = (1 - y) * 2 + x
    dg = (1 - y) * 2 + (1 - x)
    n1 = (1 - c) * xn + c * yn
    n2 = c * xn + (1 - c) * yn
    mesh_id = pl.DeviceIdType.MESH

    def weights(e, slot):
        return (
            pltpu.make_async_copy(wg.at[e], gbuf.at[slot], gsem.at[slot]),
            pltpu.make_async_copy(wu.at[e], ubuf.at[slot], usem.at[slot]),
        )

    def to(src, dst, s, r, **where):
        return pltpu.make_async_remote_copy(
            src_ref=src, dst_ref=dst, send_sem=s, recv_sem=r, device_id=where, device_id_type=mesh_id
        )

    barrier = pltpu.get_barrier_semaphore()
    peers = [dict(blk=n1), dict(blk=n2), dict(blk=dg), dict(half=1 - c)]
    peers += [dict(rep=(z + k) % reps) for k in range(1, reps)]
    for where in peers:
        pl.semaphore_signal(barrier, inc=1, device_id=where, device_id_type=mesh_id)
    pl.semaphore_wait(barrier, len(peers))

    def rows(g):
        return pl.ds(pl.multiple_of(c * H + g * R, R), R)

    s1 = [to(tok.at[rows(g)], tokb.at[0, rows(g)], t_s.at[0, g], t_r.at[0, g], blk=n1) for g in range(G)]
    s2 = [to(tok.at[rows(g)], tokb.at[1, rows(g)], t_s.at[1, g], t_r.at[1, g], blk=n2) for g in range(G)]
    s3 = [to(tokb.at[0, rows(g)], tokb.at[2, rows(g)], t_s.at[2, g], t_r.at[2, g], blk=n2) for g in range(G)]
    swap = (1, 0, 2)
    hand = [
        [to(tokb.at[k, rows(g)], tokb.at[swap[k], rows(g)], p_s.at[k, g], p_r.at[swap[k], g], half=1 - c) for g in range(G)]
        for k in range(3)
    ]

    def other_rows(g):
        return pl.ds(pl.multiple_of((1 - c) * H + g * R, R), R)

    got = [
        [to(tokb.at[swap[k], rows(g)], tokb.at[k, other_rows(g)], p_s.at[swap[k], g], p_r.at[k, g], half=1 - c) for g in range(G)]
        for k in range(3)
    ]
    metas = [
        to(meta, metab.at[k], m_s.at[k], m_r.at[k], blk=b) for k, b in enumerate((n1, n2, dg))
    ]
    for m in metas:
        m.start()
    for g in range(G):
        s1[g].start()
        s2[g].start()
    for e in range(ring):
        for w in weights(e, e):
            w.start()
    down_copy = pltpu.make_async_copy(wd, dbuf, dsem)
    down_copy.start()

    hs[...] = silu_mul(
        lax.dot_general(tok[...], sg[...], NT, preferred_element_type=F32),
        lax.dot_general(tok[...], su[...], NT, preferred_element_type=F32),
    )

    ids = (me * el + lax.broadcasted_iota(jnp.int32, (el, T), 0)).astype(F32)
    before = (
        lax.broadcasted_iota(jnp.int32, (T, T), 0) < lax.broadcasted_iota(jnp.int32, (T, T), 1)
    ).astype(F32).astype(BF)
    S = el * CAP
    spread = (
        lax.broadcasted_iota(jnp.int32, (S, el), 0) // CAP == lax.broadcasted_iota(jnp.int32, (S, el), 1)
    ).astype(F32).astype(BF)
    place = (lax.broadcasted_iota(jnp.int32, (S, T), 0) % CAP + 1).astype(F32)
    topk = meta.shape[0] // 2

    def dispatch(r, meta_ref, tok_ref):
        named = jnp.zeros((el, T), F32)
        gate = jnp.zeros((el, T), F32)
        for j in range(topk):
            hit = (meta_ref[j:j + 1, :] == ids).astype(F32)
            named = named + hit
            gate = gate + hit * meta_ref[topk + j:topk + j + 1, :]
        rank = dot(named.astype(BF), before)
        slot = dot(spread, (named * (rank + 1.0)).astype(BF))
        chosen = (slot == place).astype(F32)
        weight = chosen * dot(spread, gate.astype(BF))
        comb[r] = weight.T.astype(BF)
        pick = chosen.astype(BF)
        step = 512

        def body(k, _):
            cols = pl.ds(pl.multiple_of(k * step, step), step)
            part = dot(pick, tok_ref[:, cols]).astype(BF)
            for e in range(el):
                xs[e, r * CAP:(r + 1) * CAP, cols] = part[e * CAP:(e + 1) * CAP]
            return 0

        lax.fori_loop(0, D // step, body, 0)

    dispatch(0, meta, tok)
    for g in range(G):
        s1[g].wait_recv()
        s3[g].start()
        hand[0][g].start()
        s2[g].wait_recv()
        hand[1][g].start()
    for k in (0, 1):
        metas[k].wait_recv()
        for g in range(G):
            got[k][g].wait_recv()
        dispatch(k + 1, metab.at[k], tokb.at[k])
    for g in range(G):
        s3[g].wait_recv()
        hand[2][g].start()
    metas[2].wait_recv()
    for g in range(G):
        got[2][g].wait_recv()
    dispatch(3, metab.at[2], tokb.at[2])

    def hidden(e, slot):
        for w in weights(e, slot):
            w.wait()
        rows_e = xs[e]
        hb[e] = silu_mul(
            lax.dot_general(rows_e, gbuf[slot], NT, preferred_element_type=F32),
            lax.dot_general(rows_e, ubuf[slot], NT, preferred_element_type=F32),
        )

    def first(e, _):
        hidden(e, e)
        for w in weights(e + ring, e):
            w.start()
        return 0

    def second(e, _):
        hidden(e + ring, e)
        return 0

    lax.fori_loop(0, ring, first, 0)
    lax.fori_loop(0, ring, second, 0)
    down_copy.wait()

    def partials(offset):
        cols = pl.ds(pl.multiple_of(offset, W), W)

        def body(e, _):
            part = dot(hb[e], dbuf[e, :, cols]).astype(BF)
            at = pl.ds(pl.multiple_of(e * CAP, CAP), CAP)
            for r in range(4):
                yb[r, at, :] = part[r * CAP:(r + 1) * CAP]
            return 0

        lax.fori_loop(0, el, body, 0)
        sums = [dot(comb[r], yb[r]) for r in range(4)]
        sums[0] = sums[0] + dot(hs[...], sd[:, cols])
        return sums

    order = (0, 2, 1, 3)
    pending = []

    def run(copy):
        copy.start()
        pending.append(copy)
        return copy

    dcopy, acopy, bcopy, zcopy = {}, {}, {}, {}

    def chunk(i):
        return (z + 1 + i) % reps

    def stage_a(i):
        sums = partials(((1 - c) * reps + chunk(i)) * W)
        for r in range(4):
            dsend[i, r] = sums[r].astype(BF)
        dcopy[i] = run(to(dsend.at[i], drecv.at[i], d_s.at[i], d_r.at[i], half=1 - c))

    def stage_b(i):
        sums = partials((c * reps + chunk(i)) * W)
        for r in range(4):
            acc[r] = sums[r]
        dcopy[i].wait_recv()
        total = lambda r: acc[r] + drecv[i, order[r]].astype(F32)
        asend[i, 0] = total(1).astype(BF)
        asend[i, 1] = total(3).astype(BF)
        acopy[i] = run(to(asend.at[i], arecv.at[i], a_s.at[i], a_r.at[i], blk=n1))
        keep[i, 0] = total(0)
        keep[i, 1] = total(2)

    def stage_c(i):
        acopy[i].wait_recv()
        bsend[i] = (keep[i, 1] + arecv[i, 1].astype(F32)).astype(BF)
        bcopy[i] = run(to(bsend.at[i], brecv.at[i], b_s.at[i], b_r.at[i], blk=n2))
        keep[i, 0] = keep[i, 0] + arecv[i, 0].astype(F32)

    def stage_d(i):
        bcopy[i].wait_recv()
        whole = keep[i, 0] + brecv[i].astype(F32)
        if i < reps - 1:
            zsend[i] = whole.astype(BF)
            zcopy[i] = run(to(zsend.at[i], zrecv.at[i], z_s.at[i], z_r.at[i], rep=chunk(i)))
        else:
            for k in range(reps - 1):
                zcopy[k].wait_recv()
                whole = whole + zrecv[k].astype(F32)
            out[...] = whole.astype(out.dtype)

    for i in range(reps):
        stage_a(i)
        if i >= 1:
            stage_c(i - 1)
        stage_b(i)
        if i >= 1:
            stage_d(i - 1)
    stage_c(reps - 1)
    stage_d(reps - 1)
    for copy in pending + metas + s1 + s2 + s3 + hand[0] + hand[1] + hand[2]:
        copy.wait_send()


def fused(tokens, experts, gates, w_gate, w_up, w_down, shared_gate, shared_up, shared_down):
    T, D = tokens.shape
    el, F, _ = w_gate.shape
    reps = lax.axis_size("rep")
    W = D // (2 * reps)
    G = 2
    ring = el // 2
    meta = jnp.concatenate([experts.T.astype(F32), gates.T.astype(F32)], axis=0)
    vm = pl.BlockSpec(memory_space=pltpu.VMEM)
    hbm = pl.BlockSpec(memory_space=pl.ANY)
    dma = pltpu.SemaphoreType.DMA
    return pl.pallas_call(
        fused_kernel,
        out_shape=jax.ShapeDtypeStruct((T, W), BF),
        in_specs=[vm] * 5 + [hbm] * 3,
        out_specs=vm,
        scratch_shapes=[
            pltpu.VMEM((3, T, D), BF),
            pltpu.VMEM((3,) + meta.shape, F32),
            pltpu.VMEM((el, 4 * CAP, D), BF),
            pltpu.VMEM((el, 4 * CAP, F), BF),
            pltpu.VMEM((T, F), BF),
            pltpu.VMEM((4, T, el * CAP), BF),
            pltpu.VMEM((4, el * CAP, W), BF),
            pltpu.VMEM((ring, F, D), BF),
            pltpu.VMEM((ring, F, D), BF),
            pltpu.VMEM((el, F, D), BF),
            pltpu.VMEM((4, T, W), F32),
            pltpu.VMEM((reps, 2, T, W), F32),
            pltpu.VMEM((reps, 4, T, W), BF),
            pltpu.VMEM((reps, 4, T, W), BF),
            pltpu.VMEM((reps, 2, T, W), BF),
            pltpu.VMEM((reps, 2, T, W), BF),
            pltpu.VMEM((reps, T, W), BF),
            pltpu.VMEM((reps, T, W), BF),
            pltpu.VMEM((reps - 1, T, W), BF),
            pltpu.VMEM((reps - 1, T, W), BF),
            dma((ring,)), dma((ring,)), dma,
            dma((3, G)), dma((3, G)), dma((3, G)), dma((3, G)),
            dma((3,)), dma((3,)),
            dma((reps,)), dma((reps,)), dma((reps,)), dma((reps,)), dma((reps,)), dma((reps,)),
            dma((reps - 1,)), dma((reps - 1,)),
        ],
        compiler_params=pltpu.CompilerParams(
            collective_id=0, has_side_effects=True, vmem_limit_bytes=64 * 1024 * 1024 - 65536
        ),
    )(tokens, meta, shared_gate, shared_up, shared_down, w_gate, w_up, w_down)


def solution(mesh):
    small = mesh.shape["blk"] == 4 and mesh.shape["half"] == 2
    return jax.shard_map(
        fused if small else per_device,
        mesh=mesh,
        in_specs=(
            P("blk", None),
            P("blk", None),
            P("blk", None),
            P("blk", ("half", "rep"), None),
            P("blk", ("half", "rep"), None),
            P("blk", ("half", "rep"), None),
            P(("half", "rep"), None),
            P(("half", "rep"), None),
            P(("half", "rep"), None),
        ),
        out_specs=P("blk", ("half", "rep")),
        check_vma=False,
    )
```

```python
import functools

import jax
import jax.numpy as jnp
from jax import lax
from jax.experimental import pallas as pl
from jax.experimental.pallas import tpu as pltpu
from jax.sharding import PartitionSpec as P

E = 64
CAP = 32


def hidden_units(token_rows, gate_matrix, up_weight):
    gate_values = jnp.einsum(
        "kan,ktn->kat", token_rows, gate_matrix, preferred_element_type=jnp.float32
    )
    raised_rows = jnp.einsum(
        "kan,ktn->kat", token_rows, up_weight, preferred_element_type=jnp.float32
    )
    return (jax.nn.silu(gate_values) * raised_rows).astype(jnp.bfloat16)


def place_slots(flat, ranks, block_size, which, slot_count):
    inside = ranks // block_size == which
    local = jnp.where(inside, flat * block_size + ranks % block_size, -1)
    return local[:, None] == jnp.arange(slot_count, dtype=jnp.int32)[None, :]


def per_device(tokens, experts, gates, w_gate, w_up, w_down, shared_gate, shared_up, shared_down):
    token_count = tokens.shape[0]
    width = tokens.shape[1]
    topk = experts.shape[1]
    exp_local = w_gate.shape[0]
    blk_count = lax.axis_size("blk")
    slot_block = CAP // lax.axis_size("rep")
    member_rep = lax.axis_index("rep")
    flat = experts.reshape(-1)
    onehot = (flat[:, None] == jnp.arange(E, dtype=jnp.int32)[None, :]).astype(jnp.int32)
    before = jnp.cumsum(onehot, axis=0) - onehot
    ranks = jnp.sum(before * onehot, axis=1)
    placing = place_slots(flat, ranks, slot_block, member_rep, E * slot_block).reshape(
        token_count, topk, -1
    )
    weighting = jnp.sum(
        placing.astype(jnp.float32) * gates.astype(jnp.float32)[:, :, None], axis=1
    ).astype(jnp.bfloat16)
    selector = jnp.any(placing, axis=1).astype(jnp.bfloat16)
    filled = jnp.einsum("ts,td->sd", selector, tokens, preferred_element_type=jnp.float32).astype(
        jnp.bfloat16
    )
    filled = filled.reshape(E, 1, slot_block, width)
    arrived = lax.all_to_all(filled, "blk", split_axis=0, concat_axis=1, tiled=True)
    token_rows = arrived.reshape(exp_local, -1, width)
    every_hidden = hidden_units(lax.all_gather(token_rows, "rep", axis=1, tiled=True), w_gate, w_up)
    mine = lax.all_to_all(every_hidden, "rep", split_axis=1, concat_axis=2, tiled=True)
    partial_value = jnp.einsum(
        "otv,ovj->otj",
        mine,
        lax.all_gather(w_down, "rep", axis=1, tiled=True),
        preferred_element_type=jnp.float32,
    )
    block_out = partial_value.astype(jnp.bfloat16).reshape(exp_local, blk_count, slot_block, width)
    returned = lax.all_to_all(block_out, "blk", split_axis=1, concat_axis=0, tiled=True)
    returned = returned.reshape(E * slot_block, width)
    routed = jnp.dot(weighting, returned, preferred_element_type=jnp.float32)
    shared_hidden = (
        jax.nn.silu(
            jnp.einsum("td,sd->ts", tokens, shared_gate, preferred_element_type=jnp.float32)
        )
        * jnp.einsum("td,sd->ts", tokens, shared_up, preferred_element_type=jnp.float32)
    ).astype(jnp.bfloat16)
    shared_output = jnp.dot(shared_hidden, shared_down, preferred_element_type=jnp.float32)
    routed_share = lax.psum_scatter(routed, ("half", "rep"), scatter_dimension=1, tiled=True)
    shared_share = lax.psum_scatter(shared_output, ("half", "rep"), scatter_dimension=1, tiled=True)
    total = routed_share + shared_share
    return total.astype(jnp.bfloat16)


BF = jnp.bfloat16
F32 = jnp.float32
NT = (((1,), (1,)), ((), ()))


def dot(a, b):
    return jnp.dot(a, b, preferred_element_type=F32)


def silu_mul(g, u):
    return (g / (1.0 + jnp.exp(-g)) * u).astype(BF)


def fused_kernel(
    tok, meta, sg, su, sd, wg, wu, wd, out,
    tokb, metab, xs, hb, hs, comb, yb, gbuf, ubuf, dbuf,
    acc, keep, dsend, drecv, asend, arecv, bsend, brecv, zsend, zrecv,
    gsem, usem, dsem, t_s, t_r, p_s, p_r, m_s, m_r, d_s, d_r, a_s, a_r, b_s, b_r, z_s, z_r,
):
    T, D = tok.shape
    el, F, _ = wg.shape
    ring = gbuf.shape[0]
    W = out.shape[1]
    reps = D // (2 * W)
    H = T // 2
    G = t_s.shape[1]
    R = H // G
    me = lax.axis_index("blk")
    c = lax.axis_index("half")
    z = lax.axis_index("rep")
    x = me % 2
    y = me // 2
    xn = y * 2 + (1 - x)
    yn = (1 - y) * 2 + x
    dg = (1 - y) * 2 + (1 - x)
    n1 = (1 - c) * xn + c * yn
    n2 = c * xn + (1 - c) * yn
    mesh_id = pl.DeviceIdType.MESH

    def weights(e, slot):
        return (
            pltpu.make_async_copy(wg.at[e], gbuf.at[slot], gsem.at[slot]),
            pltpu.make_async_copy(wu.at[e], ubuf.at[slot], usem.at[slot]),
        )

    def to(src, dst, s, r, **where):
        return pltpu.make_async_remote_copy(
            src_ref=src, dst_ref=dst, send_sem=s, recv_sem=r, device_id=where, device_id_type=mesh_id
        )

    barrier = pltpu.get_barrier_semaphore()
    peers = [dict(blk=n1), dict(blk=n2), dict(blk=dg), dict(half=1 - c)]
    peers += [dict(rep=(z + k) % reps) for k in range(1, reps)]
    for where in peers:
        pl.semaphore_signal(barrier, inc=1, device_id=where, device_id_type=mesh_id)
    pl.semaphore_wait(barrier, len(peers))

    p = z % 2
    zp = z + 1 - 2 * p

    def piece(core, g):
        first = (p, 2, 3, 1 - p)[g]
        return pl.ds(pl.multiple_of(core * H + first * R, R), R)

    def rows(g):
        return piece(c, g)

    N = G - 1
    s1 = [to(tok.at[rows(g)], tokb.at[0, rows(g)], t_s.at[0, g], t_r.at[0, g], blk=n1) for g in range(N)]
    s2 = [to(tok.at[rows(g)], tokb.at[1, rows(g)], t_s.at[1, g], t_r.at[1, g], blk=n2) for g in range(N)]
    s3 = [to(tokb.at[0, rows(g)], tokb.at[2, rows(g)], t_s.at[2, g], t_r.at[2, g], blk=n2) for g in range(N)]
    sz = [to(tokb.at[k, rows(0)], tokb.at[k, rows(0)], t_s.at[k, N], t_r.at[k, N], rep=zp) for k in range(3)]
    swap = (1, 0, 2)
    hand = [
        [to(tokb.at[k, rows(g)], tokb.at[swap[k], rows(g)], p_s.at[k, g], p_r.at[swap[k], g], half=1 - c) for g in range(G)]
        for k in range(3)
    ]
    got = [
        [to(tokb.at[swap[k], piece(1 - c, g)], tokb.at[k, piece(1 - c, g)], p_s.at[swap[k], g], p_r.at[k, g], half=1 - c) for g in range(G)]
        for k in range(3)
    ]
    metas = [
        to(meta, metab.at[k], m_s.at[k], m_r.at[k], blk=b) for k, b in enumerate((n1, n2, dg))
    ]
    for m in metas:
        m.start()
    for g in range(N):
        s1[g].start()
        s2[g].start()
    for e in range(ring):
        for w in weights(e, e):
            w.start()
    down_copy = pltpu.make_async_copy(wd, dbuf, dsem)
    down_copy.start()

    hs[...] = silu_mul(
        lax.dot_general(tok[...], sg[...], NT, preferred_element_type=F32),
        lax.dot_general(tok[...], su[...], NT, preferred_element_type=F32),
    )

    ids = (me * el + lax.broadcasted_iota(jnp.int32, (el, T), 0)).astype(F32)
    before = (
        lax.broadcasted_iota(jnp.int32, (T, T), 0) < lax.broadcasted_iota(jnp.int32, (T, T), 1)
    ).astype(F32).astype(BF)
    S = el * CAP
    spread = (
        lax.broadcasted_iota(jnp.int32, (S, el), 0) // CAP == lax.broadcasted_iota(jnp.int32, (S, el), 1)
    ).astype(F32).astype(BF)
    place = (lax.broadcasted_iota(jnp.int32, (S, T), 0) % CAP + 1).astype(F32)
    topk = meta.shape[0] // 2

    def dispatch(r, meta_ref, tok_ref):
        named = jnp.zeros((el, T), F32)
        gate = jnp.zeros((el, T), F32)
        for j in range(topk):
            hit = (meta_ref[j:j + 1, :] == ids).astype(F32)
            named = named + hit
            gate = gate + hit * meta_ref[topk + j:topk + j + 1, :]
        rank = dot(named.astype(BF), before)
        slot = dot(spread, (named * (rank + 1.0)).astype(BF))
        chosen = (slot == place).astype(F32)
        weight = chosen * dot(spread, gate.astype(BF))
        comb[r] = weight.T.astype(BF)
        pick = chosen.astype(BF)
        step = 512

        def body(k, _):
            cols = pl.ds(pl.multiple_of(k * step, step), step)
            part = dot(pick, tok_ref[:, cols]).astype(BF)
            for e in range(el):
                xs[e, r * CAP:(r + 1) * CAP, cols] = part[e * CAP:(e + 1) * CAP]
            return 0

        lax.fori_loop(0, D // step, body, 0)

    dispatch(0, meta, tok)
    for g in range(N):
        s1[g].wait_recv()
        s3[g].start()
        if g == 0:
            sz[0].start()
        hand[0][g].start()
        s2[g].wait_recv()
        if g == 0:
            sz[1].start()
        hand[1][g].start()
    for k in (0, 1):
        sz[k].wait_recv()
        hand[k][N].start()
    s3[0].wait_recv()
    sz[2].start()
    hand[2][0].start()
    for k in (0, 1):
        metas[k].wait_recv()
        for g in range(G):
            got[k][g].wait_recv()
        dispatch(k + 1, metab.at[k], tokb.at[k])
    for g in range(1, N):
        s3[g].wait_recv()
        hand[2][g].start()
    sz[2].wait_recv()
    hand[2][N].start()
    metas[2].wait_recv()
    for g in range(G):
        got[2][g].wait_recv()
    dispatch(3, metab.at[2], tokb.at[2])

    def hidden(e, slot):
        for w in weights(e, slot):
            w.wait()
        rows_e = xs[e]
        hb[e] = silu_mul(
            lax.dot_general(rows_e, gbuf[slot], NT, preferred_element_type=F32),
            lax.dot_general(rows_e, ubuf[slot], NT, preferred_element_type=F32),
        )

    def first(e, _):
        hidden(e, e)
        for w in weights(e + ring, e):
            w.start()
        return 0

    def second(e, _):
        hidden(e + ring, e)
        return 0

    lax.fori_loop(0, ring, first, 0)
    lax.fori_loop(0, ring, second, 0)
    down_copy.wait()

    def partials(offset):
        cols = pl.ds(pl.multiple_of(offset, W), W)

        def body(e, _):
            part = dot(hb[e], dbuf[e, :, cols]).astype(BF)
            at = pl.ds(pl.multiple_of(e * CAP, CAP), CAP)
            for r in range(4):
                yb[r, at, :] = part[r * CAP:(r + 1) * CAP]
            return 0

        lax.fori_loop(0, el, body, 0)
        sums = [dot(comb[r], yb[r]) for r in range(4)]
        sums[0] = sums[0] + dot(hs[...], sd[:, cols])
        return sums

    order = (0, 2, 1, 3)
    pending = []

    def run(copy):
        copy.start()
        pending.append(copy)
        return copy

    dcopy, acopy, bcopy, zcopy = {}, {}, {}, {}

    def chunk(i):
        return (z + 1 + i) % reps

    def stage_a(i):
        sums = partials(((1 - c) * reps + chunk(i)) * W)
        for r in range(4):
            dsend[i, r] = sums[r].astype(BF)
        dcopy[i] = run(to(dsend.at[i], drecv.at[i], d_s.at[i], d_r.at[i], half=1 - c))

    def stage_b(i):
        sums = partials((c * reps + chunk(i)) * W)
        for r in range(4):
            acc[r] = sums[r]
        dcopy[i].wait_recv()
        total = lambda r: acc[r] + drecv[i, order[r]].astype(F32)
        for k, r in ((1, 3), (0, 1)):
            asend[i, k] = total(r).astype(BF)
            acopy[i, k] = run(to(asend.at[i, k], arecv.at[i, k], a_s.at[i, k], a_r.at[i, k], blk=n1))
        keep[i, 0] = total(0)
        keep[i, 1] = total(2)

    def stage_c(i):
        acopy[i, 1].wait_recv()
        bsend[i] = (keep[i, 1] + arecv[i, 1].astype(F32)).astype(BF)
        bcopy[i] = run(to(bsend.at[i], brecv.at[i], b_s.at[i], b_r.at[i], blk=n2))

    def stage_d(i):
        acopy[i, 0].wait_recv()
        bcopy[i].wait_recv()
        whole = keep[i, 0] + arecv[i, 0].astype(F32) + brecv[i].astype(F32)
        if i < reps - 1:
            zsend[i] = whole.astype(BF)
            zcopy[i] = run(to(zsend.at[i], zrecv.at[i], z_s.at[i], z_r.at[i], rep=chunk(i)))
        else:
            for k in range(reps - 1):
                zcopy[k].wait_recv()
                whole = whole + zrecv[k].astype(F32)
            out[...] = whole.astype(out.dtype)

    stage_a(0)
    for i in range(reps + 2):
        if i + 1 < reps:
            stage_a(i + 1)
        if i < reps:
            stage_b(i)
        if i == reps:
            stage_d(i - 2)
        if 0 <= i - 1 < reps:
            stage_c(i - 1)
        if 0 <= i - 2 < reps and i != reps:
            stage_d(i - 2)
    for copy in pending + metas + s1 + s2 + s3 + sz + hand[0] + hand[1] + hand[2]:
        copy.wait_send()


def fused(tokens, experts, gates, w_gate, w_up, w_down, shared_gate, shared_up, shared_down):
    T, D = tokens.shape
    el, F, _ = w_gate.shape
    reps = lax.axis_size("rep")
    W = D // (2 * reps)
    G = 4
    ring = el // 2
    meta = jnp.concatenate([experts.T.astype(F32), gates.T.astype(F32)], axis=0)
    vm = pl.BlockSpec(memory_space=pltpu.VMEM)
    hbm = pl.BlockSpec(memory_space=pl.ANY)
    dma = pltpu.SemaphoreType.DMA
    return pl.pallas_call(
        fused_kernel,
        out_shape=jax.ShapeDtypeStruct((T, W), BF),
        in_specs=[vm] * 5 + [hbm] * 3,
        out_specs=vm,
        scratch_shapes=[
            pltpu.VMEM((3, T, D), BF),
            pltpu.VMEM((3,) + meta.shape, F32),
            pltpu.VMEM((el, 4 * CAP, D), BF),
            pltpu.VMEM((el, 4 * CAP, F), BF),
            pltpu.VMEM((T, F), BF),
            pltpu.VMEM((4, T, el * CAP), BF),
            pltpu.VMEM((4, el * CAP, W), BF),
            pltpu.VMEM((ring, F, D), BF),
            pltpu.VMEM((ring, F, D), BF),
            pltpu.VMEM((el, F, D), BF),
            pltpu.VMEM((4, T, W), F32),
            pltpu.VMEM((reps, 2, T, W), F32),
            pltpu.VMEM((reps, 4, T, W), BF),
            pltpu.VMEM((reps, 4, T, W), BF),
            pltpu.VMEM((reps, 2, T, W), BF),
            pltpu.VMEM((reps, 2, T, W), BF),
            pltpu.VMEM((reps, T, W), BF),
            pltpu.VMEM((reps, T, W), BF),
            pltpu.VMEM((reps - 1, T, W), BF),
            pltpu.VMEM((reps - 1, T, W), BF),
            dma((ring,)), dma((ring,)), dma,
            dma((3, G)), dma((3, G)), dma((3, G)), dma((3, G)),
            dma((3,)), dma((3,)),
            dma((reps,)), dma((reps,)), dma((reps, 2)), dma((reps, 2)), dma((reps,)), dma((reps,)),
            dma((reps - 1,)), dma((reps - 1,)),
        ],
        compiler_params=pltpu.CompilerParams(
            collective_id=0, has_side_effects=True, vmem_limit_bytes=64 * 1024 * 1024 - 65536
        ),
    )(tokens, meta, shared_gate, shared_up, shared_down, w_gate, w_up, w_down)


def solution(mesh):
    small = mesh.shape["blk"] == 4 and mesh.shape["half"] == 2 and mesh.shape["rep"] % 2 == 0
    return jax.shard_map(
        fused if small else per_device,
        mesh=mesh,
        in_specs=(
            P("blk", None),
            P("blk", None),
            P("blk", None),
            P("blk", ("half", "rep"), None),
            P("blk", ("half", "rep"), None),
            P("blk", ("half", "rep"), None),
            P(("half", "rep"), None),
            P(("half", "rep"), None),
            P(("half", "rep"), None),
        ),
        out_specs=P("blk", ("half", "rep")),
        check_vma=False,
    )
```

```python
import functools

import jax
import jax.numpy as jnp
from jax import lax
from jax.experimental import pallas as pl
from jax.experimental.pallas import tpu as pltpu
from jax.sharding import PartitionSpec as P

E = 64
CAP = 32


def hidden_units(token_rows, gate_matrix, up_weight):
    gate_values = jnp.einsum(
        "kan,ktn->kat", token_rows, gate_matrix, preferred_element_type=jnp.float32
    )
    raised_rows = jnp.einsum(
        "kan,ktn->kat", token_rows, up_weight, preferred_element_type=jnp.float32
    )
    return (jax.nn.silu(gate_values) * raised_rows).astype(jnp.bfloat16)


def place_slots(flat, ranks, block_size, which, slot_count):
    inside = ranks // block_size == which
    local = jnp.where(inside, flat * block_size + ranks % block_size, -1)
    return local[:, None] == jnp.arange(slot_count, dtype=jnp.int32)[None, :]


def per_device(tokens, experts, gates, w_gate, w_up, w_down, shared_gate, shared_up, shared_down):
    token_count = tokens.shape[0]
    width = tokens.shape[1]
    topk = experts.shape[1]
    exp_local = w_gate.shape[0]
    blk_count = lax.axis_size("blk")
    slot_block = CAP // lax.axis_size("rep")
    member_rep = lax.axis_index("rep")
    flat = experts.reshape(-1)
    onehot = (flat[:, None] == jnp.arange(E, dtype=jnp.int32)[None, :]).astype(jnp.int32)
    before = jnp.cumsum(onehot, axis=0) - onehot
    ranks = jnp.sum(before * onehot, axis=1)
    placing = place_slots(flat, ranks, slot_block, member_rep, E * slot_block).reshape(
        token_count, topk, -1
    )
    weighting = jnp.sum(
        placing.astype(jnp.float32) * gates.astype(jnp.float32)[:, :, None], axis=1
    ).astype(jnp.bfloat16)
    selector = jnp.any(placing, axis=1).astype(jnp.bfloat16)
    filled = jnp.einsum("ts,td->sd", selector, tokens, preferred_element_type=jnp.float32).astype(
        jnp.bfloat16
    )
    filled = filled.reshape(E, 1, slot_block, width)
    arrived = lax.all_to_all(filled, "blk", split_axis=0, concat_axis=1, tiled=True)
    token_rows = arrived.reshape(exp_local, -1, width)
    every_hidden = hidden_units(lax.all_gather(token_rows, "rep", axis=1, tiled=True), w_gate, w_up)
    mine = lax.all_to_all(every_hidden, "rep", split_axis=1, concat_axis=2, tiled=True)
    partial_value = jnp.einsum(
        "otv,ovj->otj",
        mine,
        lax.all_gather(w_down, "rep", axis=1, tiled=True),
        preferred_element_type=jnp.float32,
    )
    block_out = partial_value.astype(jnp.bfloat16).reshape(exp_local, blk_count, slot_block, width)
    returned = lax.all_to_all(block_out, "blk", split_axis=1, concat_axis=0, tiled=True)
    returned = returned.reshape(E * slot_block, width)
    routed = jnp.dot(weighting, returned, preferred_element_type=jnp.float32)
    shared_hidden = (
        jax.nn.silu(
            jnp.einsum("td,sd->ts", tokens, shared_gate, preferred_element_type=jnp.float32)
        )
        * jnp.einsum("td,sd->ts", tokens, shared_up, preferred_element_type=jnp.float32)
    ).astype(jnp.bfloat16)
    shared_output = jnp.dot(shared_hidden, shared_down, preferred_element_type=jnp.float32)
    routed_share = lax.psum_scatter(routed, ("half", "rep"), scatter_dimension=1, tiled=True)
    shared_share = lax.psum_scatter(shared_output, ("half", "rep"), scatter_dimension=1, tiled=True)
    total = routed_share + shared_share
    return total.astype(jnp.bfloat16)


BF = jnp.bfloat16
F32 = jnp.float32
NT = (((1,), (1,)), ((), ()))


def dot(a, b):
    return jnp.dot(a, b, preferred_element_type=F32)


def silu_mul(g, u):
    return (g / (1.0 + jnp.exp(-g)) * u).astype(BF)


def fused_kernel(
    tok, meta, sg, su, sd, wg, wu, wd, out,
    tokb, metab, xs, hb, hs, comb, yb, gbuf, ubuf, dbuf,
    acc, keep, dsend, drecv, asend, arecv, bsend, brecv, zsend, zrecv,
    gsem, usem, dsem, t_s, t_r, p_s, p_r, m_s, m_r, d_s, d_r, a_s, a_r, b_s, b_r, z_s, z_r,
):
    T, D = tok.shape
    el, F, _ = wg.shape
    ring = gbuf.shape[0]
    W = out.shape[1]
    reps = D // (2 * W)
    H = T // 2
    G = t_s.shape[1]
    R = H // G
    me = lax.axis_index("blk")
    c = lax.axis_index("half")
    z = lax.axis_index("rep")
    x = me % 2
    y = me // 2
    xn = y * 2 + (1 - x)
    yn = (1 - y) * 2 + x
    dg = (1 - y) * 2 + (1 - x)
    n1 = (1 - c) * xn + c * yn
    n2 = c * xn + (1 - c) * yn
    mesh_id = pl.DeviceIdType.MESH

    def weights(e, slot):
        return (
            pltpu.make_async_copy(wg.at[e], gbuf.at[slot], gsem.at[slot]),
            pltpu.make_async_copy(wu.at[e], ubuf.at[slot], usem.at[slot]),
        )

    def to(src, dst, s, r, **where):
        return pltpu.make_async_remote_copy(
            src_ref=src, dst_ref=dst, send_sem=s, recv_sem=r, device_id=where, device_id_type=mesh_id
        )

    barrier = pltpu.get_barrier_semaphore()
    peers = [dict(blk=n1), dict(blk=n2), dict(blk=dg), dict(half=1 - c)]
    peers += [dict(rep=(z + k) % reps) for k in range(1, reps)]
    for where in peers:
        pl.semaphore_signal(barrier, inc=1, device_id=where, device_id_type=mesh_id)
    pl.semaphore_wait(barrier, len(peers))

    p = z % 2
    zp = z + 1 - 2 * p

    def piece(core, g):
        first = (p, 2, 3, 1 - p)[g]
        return pl.ds(pl.multiple_of(core * H + first * R, R), R)

    def rows(g):
        return piece(c, g)

    N = G - 1
    s1 = [to(tok.at[rows(g)], tokb.at[0, rows(g)], t_s.at[0, g], t_r.at[0, g], blk=n1) for g in range(N)]
    s2 = [to(tok.at[rows(g)], tokb.at[1, rows(g)], t_s.at[1, g], t_r.at[1, g], blk=n2) for g in range(N)]
    s3 = [to(tokb.at[0, rows(g)], tokb.at[2, rows(g)], t_s.at[2, g], t_r.at[2, g], blk=n2) for g in range(N)]
    sz = [to(tokb.at[k, rows(0)], tokb.at[k, rows(0)], t_s.at[k, N], t_r.at[k, N], rep=zp) for k in range(3)]
    swap = (1, 0, 2)
    hand = [
        [to(tokb.at[k, rows(g)], tokb.at[swap[k], rows(g)], p_s.at[k, g], p_r.at[swap[k], g], half=1 - c) for g in range(G)]
        for k in range(3)
    ]
    got = [
        [to(tokb.at[swap[k], piece(1 - c, g)], tokb.at[k, piece(1 - c, g)], p_s.at[swap[k], g], p_r.at[k, g], half=1 - c) for g in range(G)]
        for k in range(3)
    ]
    metas = [
        to(meta, metab.at[k], m_s.at[k], m_r.at[k], blk=b) for k, b in enumerate((n1, n2, dg))
    ]
    for m in metas:
        m.start()
    for g in range(N):
        s1[g].start()
        s2[g].start()
    for e in range(ring):
        for w in weights(e, e):
            w.start()
    down_copy = pltpu.make_async_copy(wd, dbuf, dsem)
    down_copy.start()

    hs[...] = silu_mul(
        lax.dot_general(tok[...], sg[...], NT, preferred_element_type=F32),
        lax.dot_general(tok[...], su[...], NT, preferred_element_type=F32),
    )

    ids = (me * el + lax.broadcasted_iota(jnp.int32, (el, T), 0)).astype(F32)
    before = (
        lax.broadcasted_iota(jnp.int32, (T, T), 0) < lax.broadcasted_iota(jnp.int32, (T, T), 1)
    ).astype(F32).astype(BF)
    S = el * CAP
    spread = (
        lax.broadcasted_iota(jnp.int32, (S, el), 0) // CAP == lax.broadcasted_iota(jnp.int32, (S, el), 1)
    ).astype(F32).astype(BF)
    place = (lax.broadcasted_iota(jnp.int32, (S, T), 0) % CAP + 1).astype(F32)
    topk = meta.shape[0] // 2

    def dispatch(r, meta_ref, tok_ref):
        named = jnp.zeros((el, T), F32)
        gate = jnp.zeros((el, T), F32)
        for j in range(topk):
            hit = (meta_ref[j:j + 1, :] == ids).astype(F32)
            named = named + hit
            gate = gate + hit * meta_ref[topk + j:topk + j + 1, :]
        rank = dot(named.astype(BF), before)
        slot = dot(spread, (named * (rank + 1.0)).astype(BF))
        chosen = (slot == place).astype(F32)
        weight = chosen * dot(spread, gate.astype(BF))
        comb[r] = weight.T.astype(BF)
        pick = chosen.astype(BF)
        step = 512

        def body(k, _):
            cols = pl.ds(pl.multiple_of(k * step, step), step)
            part = dot(pick, tok_ref[:, cols]).astype(BF)
            for e in range(el):
                xs[e, r * CAP:(r + 1) * CAP, cols] = part[e * CAP:(e + 1) * CAP]
            return 0

        lax.fori_loop(0, D // step, body, 0, unroll=1)

    dispatch(0, meta, tok)
    for g in range(N):
        s1[g].wait_recv()
        s3[g].start()
        if g == 0:
            sz[0].start()
        hand[0][g].start()
        s2[g].wait_recv()
        if g == 0:
            sz[1].start()
        hand[1][g].start()
    for k in (0, 1):
        sz[k].wait_recv()
        hand[k][N].start()
    s3[0].wait_recv()
    sz[2].start()
    hand[2][0].start()
    for k in (0, 1):
        metas[k].wait_recv()
        for g in range(G):
            got[k][g].wait_recv()
        dispatch(k + 1, metab.at[k], tokb.at[k])
    for g in range(1, N):
        s3[g].wait_recv()
        hand[2][g].start()
    sz[2].wait_recv()
    hand[2][N].start()
    metas[2].wait_recv()
    for g in range(G):
        got[2][g].wait_recv()
    dispatch(3, metab.at[2], tokb.at[2])

    def hidden(e, slot):
        for w in weights(e, slot):
            w.wait()
        rows_e = xs[e]
        hb[e] = silu_mul(
            lax.dot_general(rows_e, gbuf[slot], NT, preferred_element_type=F32),
            lax.dot_general(rows_e, ubuf[slot], NT, preferred_element_type=F32),
        )

    def first(e, _):
        hidden(e, e)
        for w in weights(e + ring, e):
            w.start()
        return 0

    def second(e, _):
        hidden(e + ring, e)
        return 0

    lax.fori_loop(0, ring, first, 0, unroll=4)
    lax.fori_loop(0, ring, second, 0, unroll=4)
    down_copy.wait()

    def partials(offset):
        cols = pl.ds(pl.multiple_of(offset, W), W)

        def body(e, _):
            part = dot(hb[e], dbuf[e, :, cols]).astype(BF)
            at = pl.ds(pl.multiple_of(e * CAP, CAP), CAP)
            for r in range(4):
                yb[r, at, :] = part[r * CAP:(r + 1) * CAP]
            return 0

        lax.fori_loop(0, el, body, 0, unroll=8)
        sums = [dot(comb[r], yb[r]) for r in range(4)]
        sums[0] = sums[0] + dot(hs[...], sd[:, cols])
        return sums

    order = (0, 2, 1, 3)
    pending = []

    def run(copy):
        copy.start()
        pending.append(copy)
        return copy

    dcopy, acopy, bcopy, zcopy = {}, {}, {}, {}

    def chunk(i):
        return (z + 1 + i) % reps

    def stage_a(i):
        sums = partials(((1 - c) * reps + chunk(i)) * W)
        for r in range(4):
            dsend[i, r] = sums[r].astype(BF)
        dcopy[i] = run(to(dsend.at[i], drecv.at[i], d_s.at[i], d_r.at[i], half=1 - c))

    def stage_b(i):
        sums = partials((c * reps + chunk(i)) * W)
        for r in range(4):
            acc[r] = sums[r]
        dcopy[i].wait_recv()
        total = lambda r: acc[r] + drecv[i, order[r]].astype(F32)
        for k, r in ((1, 3), (0, 1)):
            asend[i, k] = total(r).astype(BF)
            acopy[i, k] = run(to(asend.at[i, k], arecv.at[i, k], a_s.at[i, k], a_r.at[i, k], blk=n1))
        keep[i, 0] = total(0)
        keep[i, 1] = total(2)

    def stage_c(i):
        acopy[i, 1].wait_recv()
        bsend[i] = (keep[i, 1] + arecv[i, 1].astype(F32)).astype(BF)
        bcopy[i] = run(to(bsend.at[i], brecv.at[i], b_s.at[i], b_r.at[i], blk=n2))

    def stage_d(i):
        acopy[i, 0].wait_recv()
        bcopy[i].wait_recv()
        whole = keep[i, 0] + arecv[i, 0].astype(F32) + brecv[i].astype(F32)
        if i < reps - 1:
            zsend[i] = whole.astype(BF)
            zcopy[i] = run(to(zsend.at[i], zrecv.at[i], z_s.at[i], z_r.at[i], rep=chunk(i)))
        else:
            for k in range(reps - 1):
                zcopy[k].wait_recv()
                whole = whole + zrecv[k].astype(F32)
            out[...] = whole.astype(out.dtype)

    stage_a(0)
    for i in range(reps + 2):
        if i + 1 < reps:
            stage_a(i + 1)
        if i < reps:
            stage_b(i)
        if i == reps:
            stage_d(i - 2)
        if 0 <= i - 1 < reps:
            stage_c(i - 1)
        if 0 <= i - 2 < reps and i != reps:
            stage_d(i - 2)
    for copy in pending + metas + s1 + s2 + s3 + sz + hand[0] + hand[1] + hand[2]:
        copy.wait_send()


def fused(tokens, experts, gates, w_gate, w_up, w_down, shared_gate, shared_up, shared_down):
    T, D = tokens.shape
    el, F, _ = w_gate.shape
    reps = lax.axis_size("rep")
    W = D // (2 * reps)
    G = 4
    ring = el // 2
    meta = jnp.concatenate([experts.T.astype(F32), gates.T.astype(F32)], axis=0)
    vm = pl.BlockSpec(memory_space=pltpu.VMEM)
    hbm = pl.BlockSpec(memory_space=pl.ANY)
    dma = pltpu.SemaphoreType.DMA
    return pl.pallas_call(
        fused_kernel,
        out_shape=jax.ShapeDtypeStruct((T, W), BF),
        in_specs=[vm] * 5 + [hbm] * 3,
        out_specs=vm,
        scratch_shapes=[
            pltpu.VMEM((3, T, D), BF),
            pltpu.VMEM((3,) + meta.shape, F32),
            pltpu.VMEM((el, 4 * CAP, D), BF),
            pltpu.VMEM((el, 4 * CAP, F), BF),
            pltpu.VMEM((T, F), BF),
            pltpu.VMEM((4, T, el * CAP), BF),
            pltpu.VMEM((4, el * CAP, W), BF),
            pltpu.VMEM((ring, F, D), BF),
            pltpu.VMEM((ring, F, D), BF),
            pltpu.VMEM((el, F, D), BF),
            pltpu.VMEM((4, T, W), F32),
            pltpu.VMEM((reps, 2, T, W), F32),
            pltpu.VMEM((reps, 4, T, W), BF),
            pltpu.VMEM((reps, 4, T, W), BF),
            pltpu.VMEM((reps, 2, T, W), BF),
            pltpu.VMEM((reps, 2, T, W), BF),
            pltpu.VMEM((reps, T, W), BF),
            pltpu.VMEM((reps, T, W), BF),
            pltpu.VMEM((reps - 1, T, W), BF),
            pltpu.VMEM((reps - 1, T, W), BF),
            dma((ring,)), dma((ring,)), dma,
            dma((3, G)), dma((3, G)), dma((3, G)), dma((3, G)),
            dma((3,)), dma((3,)),
            dma((reps,)), dma((reps,)), dma((reps, 2)), dma((reps, 2)), dma((reps,)), dma((reps,)),
            dma((reps - 1,)), dma((reps - 1,)),
        ],
        compiler_params=pltpu.CompilerParams(
            collective_id=0, has_side_effects=True, vmem_limit_bytes=64 * 1024 * 1024 - 65536
        ),
    )(tokens, meta, shared_gate, shared_up, shared_down, w_gate, w_up, w_down)


def solution(mesh):
    small = mesh.shape["blk"] == 4 and mesh.shape["half"] == 2 and mesh.shape["rep"] % 2 == 0
    return jax.shard_map(
        fused if small else per_device,
        mesh=mesh,
        in_specs=(
            P("blk", None),
            P("blk", None),
            P("blk", None),
            P("blk", ("half", "rep"), None),
            P("blk", ("half", "rep"), None),
            P("blk", ("half", "rep"), None),
            P(("half", "rep"), None),
            P(("half", "rep"), None),
            P(("half", "rep"), None),
        ),
        out_specs=P("blk", ("half", "rep")),
        check_vma=False,
    )
```
